32 devices in a mesh: dp: 8 (over z, core), tensor: 4 (over y, x).
Axes of the slice: x: 2, y: 2, z: 4, core: 2. Of those that a mesh axis runs over, the one named last changes fastest.
Arguments:
- latents: bfloat16 [88, 256, 640], P('dp', 'tensor'), may hold values from -6 to 6
- cotangent: bfloat16 [88, 256, 640], P('dp', 'tensor'), may hold values from -6 to 6
- trunc_steps: int32 [8], replicated, may hold values from 30 to 40, as said below
- timesteps: int32 [88], replicated, may hold values from 100 to 900
- tile_map: int32 [88], replicated, may hold values from 0 to 87, as said below
- gain: float32 [640], replicated, may hold values from 0.5 to 1.5
- w_value: bfloat16 [640, 2560], P(None, 'tensor'), may hold values from -0.25 to 0.25
- w_gate: bfloat16 [640, 2560], P(None, 'tensor'), may hold values from -0.25 to 0.25
- w_out: bfloat16 [640, 2560], P(None, 'tensor'), may hold values from -0.125 to 0.125
Outputs:
- placed_grad: bfloat16 [88, 256, 640], P('dp', 'tensor')
- grad_value: float32 [640, 2560], P('dp', 'tensor')
- grad_gate: float32 [640, 2560], P('dp', 'tensor')
- grad_out_proj: float32 [640, 2560], P('dp', 'tensor')
- grad_gain: float32 [640], replicated
The draws below stay inside these ranges and needn't reach their ends.
Inputs may be any that keep to these rules, and one draw needn't show every extreme that they name: trunc_steps lies in 30 to 40, so a prompt has 1 to 11 live slots, its lowest ones. tile_map is a permutation of 0 to 87. Output slots g * 11 to g * 11 + 10 form group g; the live items go to the lowest slots of the groups, and each group receives the floor or the ceiling of (number of live items) / 8 of them.
All inputs are finite; a program needn't handle non-finite values.
Results may differ from the reference program's by a relative error of at most 0.0068.
Values may be sent and summed in bfloat16 or wider, within the bound.
A program may use at most 64 MiB of HBM per device.

```python
import jax
import jax.numpy as jnp
from jax import lax

C = 640
FI = 2560
ROWS = 256
SLOTS = 11
PROMPTS = 8
ITEMS = 88


def chain_plan(key):
    steps = jax.random.randint(jax.random.fold_in(key, 11), (PROMPTS,), 30, 41).astype(jnp.int32)
    item_ids = jnp.arange(ITEMS, dtype=jnp.int32)
    live = (item_ids % SLOTS < jnp.repeat(steps, SLOTS) - 29).astype(jnp.int32)
    shuffled = jax.random.permutation(jax.random.fold_in(key, 12), ITEMS).astype(jnp.int32)
    ranking = (1 - live) * ITEMS + shuffled
    ordering = jnp.argsort(ranking, stable=True).astype(jnp.int32)
    groups = ITEMS // SLOTS
    slot_of = item_ids % groups * SLOTS + item_ids // groups
    tile_map = jnp.zeros((ITEMS,), jnp.int32).at[ordering].set(slot_of.astype(jnp.int32))
    return (steps, tile_map)


def draw_trunc_steps(key, part):
    return chain_plan(key)[0]


def draw_tile_map(key, part):
    return chain_plan(key)[1]


def with_ends(result, own_key, low, top_value):
    longest = result.shape.index(max(result.shape))
    spots = []
    for shift in (0, 1):
        where = [jax.random.randint(jax.random.fold_in(own_key, axis), (), 0, length) for axis, length in enumerate(result.shape)]
        where[longest] = (where[longest] + shift) % result.shape[longest]
        spots.append(tuple(where))
    return result.at[spots[0]].set(low).at[spots[1]].set(top_value)


def block_scale(rng, extent, cuts, low, high):
    def one(dim, parts):
        draws = jax.random.uniform(jax.random.fold_in(jax.random.fold_in(rng, 6), dim), (parts,), jnp.float32, low / len(cuts), high / len(cuts))
        return jnp.repeat(jnp.exp(draws), extent[dim] // parts).reshape((-1,) + (1,) * (len(extent) - dim - 1))

    level = one(*cuts[0])
    for cut in cuts[1:]:
        level = level * one(*cut)
    return level


def bell_draw(stream_key, dims, scale, reach, cuts=(), held_as=jnp.bfloat16):
    drawn = scale * jax.random.normal(stream_key, dims, jnp.float32)
    if cuts:
        drawn = drawn * block_scale(stream_key, dims, cuts, -0.22, 0.18)
    return jnp.clip(drawn, -reach, reach).astype(held_as)


def setup_inputs(seed: int = 0) -> dict:
    key_of = jax.random.split(jax.random.key(seed), 10)
    return {
        "latents": bell_draw(key_of[0], (ITEMS, ROWS, C), 1.0, 6.0, ((0, 8), (1, 4))),
        "cotangent": bell_draw(key_of[1], (ITEMS, ROWS, C), 1.0, 6.0, ((0, 8), (1, 4))),
        "trunc_steps": draw_trunc_steps(jax.random.fold_in(key_of[9], 71), 0),
        "timesteps": with_ends(jax.random.randint(key_of[3], (ITEMS,), 100, 901), jax.random.fold_in(key_of[3], 1), 100, 900).astype(jnp.int32),
        "tile_map": draw_tile_map(jax.random.fold_in(key_of[9], 71), 0),
        "gain": jnp.clip(1.0 + 0.1 * jax.random.normal(key_of[5], (C,), jnp.float32), 0.5, 1.5),
        "w_value": bell_draw(key_of[6], (C, FI), C ** -0.5, 0.25, ((1, 4),)),
        "w_gate": bell_draw(key_of[7], (C, FI), C ** -0.5, 0.25, ((1, 4),)),
        "w_out": bell_draw(key_of[8], (C, FI), FI ** -0.5, 0.125, ((1, 4),)),
    }


eps = 1e-05

def alpha_bars():
    betas = jnp.linspace(0.00085 ** 0.5, 0.012 ** 0.5, 1000, dtype=jnp.float32) ** 2
    return jnp.exp(jnp.cumsum(jnp.log1p(-betas)))

def gelu_parts(inputs):
    cdf = 0.5 * (1.0 + lax.erf(inputs * 0.7071067811865476))
    density = jnp.exp(-0.5 * inputs * inputs) * 0.3989422804014327
    return (inputs * cdf, cdf + inputs * density)

def item_backward(normed, grad_tile, w_value, w_gate, w_out):
    values_proj = jnp.dot(normed, w_value, preferred_element_type=jnp.float32)
    gate_proj = jnp.dot(normed, w_gate, preferred_element_type=jnp.float32)
    gelu_gate, gelu_slope = gelu_parts(gate_proj)
    hidden = (values_proj * gelu_gate).astype(jnp.bfloat16)
    d_hidden = jnp.dot(grad_tile, w_out, preferred_element_type=jnp.float32)
    d_value = (d_hidden * gelu_gate).astype(jnp.bfloat16)
    d_gate = (d_hidden * values_proj * gelu_slope).astype(jnp.bfloat16)
    first_dims = (((0,), (0,)), ((), ()))
    last_dims = (((1,), (1,)), ((), ()))
    grad_wv = lax.dot_general(normed, d_value, first_dims, preferred_element_type=jnp.float32)
    grad_wg = lax.dot_general(normed, d_gate, first_dims, preferred_element_type=jnp.float32)
    grad_wo = lax.dot_general(grad_tile, hidden, first_dims, preferred_element_type=jnp.float32)
    d_normed = lax.dot_general(d_value, w_value, last_dims, preferred_element_type=jnp.float32)
    d_normed = d_normed + lax.dot_general(d_gate, w_gate, last_dims, preferred_element_type=jnp.float32)
    return (grad_wv, grad_wg, grad_wo, d_normed)

def reference(latents, cotangent, trunc_steps, timesteps, tile_map, gain, w_value, w_gate, w_out):
    total = latents.shape[0]
    item_ids = jnp.arange(total, dtype=jnp.int32)
    live = item_ids % SLOTS < jnp.repeat(trunc_steps, SLOTS) - 29
    noise_scale = jnp.sqrt(1.0 - alpha_bars()[timesteps])
    width = latents.shape[2]
    inner = w_value.shape[1]

    def one_item(carry, inputs):
        tile, cot_tile, item_scale, is_live = inputs
        x_float = tile.astype(jnp.float32)
        row_mean = lax.optimization_barrier(jnp.mean(x_float, axis=-1, keepdims=True))
        centred = x_float - row_mean
        row_var = lax.optimization_barrier(jnp.mean(centred * centred, axis=-1, keepdims=True))
        inv_std = lax.rsqrt(row_var + eps)
        x_hat = centred * inv_std
        normed = (x_hat * gain).astype(jnp.bfloat16)
        grad_tile = (cot_tile.astype(jnp.float32) * item_scale).astype(jnp.bfloat16)

        def run(unused):
            grad_wv, grad_wg, grad_wo, d_normed = item_backward(normed, grad_tile, w_value, w_gate, w_out)
            d_hat = d_normed * gain
            input_grad = grad_tile.astype(jnp.float32) + inv_std * (d_hat - lax.optimization_barrier(jnp.mean(d_hat, axis=-1, keepdims=True)) - x_hat * lax.optimization_barrier(jnp.mean(d_hat * x_hat, axis=-1, keepdims=True)))
            gain_part = lax.optimization_barrier(jnp.sum(d_normed * x_hat, axis=0))
            return (grad_wv, grad_wg, grad_wo, gain_part, input_grad.astype(jnp.bfloat16))

        def skip(unused):
            zero_w = jnp.zeros((width, inner), jnp.float32)
            return (zero_w, zero_w, zero_w, jnp.zeros((width,), jnp.float32), jnp.zeros(tile.shape, jnp.bfloat16))
        grad_wv, grad_wg, grad_wo, gain_part, input_grad = lax.cond(is_live, run, skip, None)
        carry = (carry[0] + grad_wv, carry[1] + grad_wg, carry[2] + grad_wo, carry[3] + gain_part)
        return (carry, input_grad)
    zero_w = jnp.zeros((width, inner), jnp.float32)
    init = (zero_w, zero_w, zero_w, jnp.zeros((width,), jnp.float32))
    sums, input_grads = lax.scan(one_item, init, (latents, cotangent, noise_scale, live))
    placed_grad = jnp.zeros(latents.shape, jnp.bfloat16).at[tile_map.astype(jnp.int32)].set(input_grads)
    return (placed_grad, sums[0], sums[1], sums[2], sums[3])
```

```python
import functools

import jax
import jax.numpy as jnp
import numpy as np
from jax import lax
from jax.experimental import pallas as pl
from jax.experimental.pallas import tpu as pltpu
from jax.sharding import PartitionSpec as P

eps = 1e-05


def noise_table():
    betas = np.linspace(0.00085**0.5, 0.012**0.5, 1000) ** 2
    abar = np.exp(np.cumsum(np.log1p(-betas)))
    return np.sqrt(1.0 - abar).astype(np.float32)


def block_kernel(live_ref, scale_ref, x_ref, cot_ref, gain_ref, wv_ref, wg_ref, wo_ref,
                 dn_ref, dw_ref, acc_v, acc_g, acc_o):
    step = pl.program_id(0)
    inner = wv_ref.shape[1]
    first = (((0,), (0,)), ((), ()))
    last = (((1,), (1,)), ((), ()))

    @pl.when(step == 0)
    def _():
        acc_v[...] = jnp.zeros_like(acc_v)
        acc_g[...] = jnp.zeros_like(acc_g)
        acc_o[...] = jnp.zeros_like(acc_o)

    @pl.when(step < live_ref[0])
    def _():
        x = x_ref[0].astype(jnp.float32)
        centred = x - jnp.mean(x, axis=-1, keepdims=True)
        inv_std = lax.rsqrt(jnp.mean(centred * centred, axis=-1, keepdims=True) + eps)
        normed = (centred * inv_std * gain_ref[...]).astype(jnp.bfloat16)
        grad = (cot_ref[0].astype(jnp.float32) * scale_ref[step]).astype(jnp.bfloat16)
        values = jnp.dot(normed, wv_ref[...], preferred_element_type=jnp.float32)
        gate = jnp.dot(normed, wg_ref[...], preferred_element_type=jnp.float32)
        d_hidden = jnp.dot(grad, wo_ref[...], preferred_element_type=jnp.float32)
        cdf = 0.5 * (1.0 + lax.erf(gate * 0.7071067811865476))
        density = jnp.exp(-0.5 * gate * gate) * 0.3989422804014327
        gelu = gate * cdf
        hidden = (values * gelu).astype(jnp.bfloat16)
        d_value = (d_hidden * gelu).astype(jnp.bfloat16)
        d_gate = (d_hidden * values * (cdf + gate * density)).astype(jnp.bfloat16)
        acc_v[...] += lax.dot_general(normed, d_value, first, preferred_element_type=jnp.float32)
        acc_g[...] += lax.dot_general(normed, d_gate, first, preferred_element_type=jnp.float32)
        acc_o[...] += lax.dot_general(grad, hidden, first, preferred_element_type=jnp.float32)
        d_normed = lax.dot_general(d_value, wv_ref[...], last, preferred_element_type=jnp.float32)
        d_normed += lax.dot_general(d_gate, wg_ref[...], last, preferred_element_type=jnp.float32)
        dn_ref[0] = d_normed.astype(jnp.bfloat16)

    @pl.when(step == pl.num_programs(0) - 1)
    def _():
        dw_ref[:, 0:inner] = acc_v[...].astype(jnp.bfloat16)
        dw_ref[:, inner : 2 * inner] = acc_g[...].astype(jnp.bfloat16)
        dw_ref[:, 2 * inner : 3 * inner] = acc_o[...].astype(jnp.bfloat16)


def block_backward(live, scale, x, cot, gain, w_value, w_gate, w_out):
    slots, rows, width = x.shape
    inner = w_value.shape[1]

    def tile(t, live_ref, scale_ref):
        return (jnp.minimum(t, live_ref[0] - 1), 0, 0)

    def whole(t, live_ref, scale_ref):
        return (0, 0)

    weight = pl.BlockSpec((width, inner), whole)
    return pl.pallas_call(
        block_kernel,
        grid_spec=pltpu.PrefetchScalarGridSpec(
            num_scalar_prefetch=2,
            grid=(slots,),
            in_specs=[
                pl.BlockSpec((1, rows, width), tile),
                pl.BlockSpec((1, rows, width), tile),
                pl.BlockSpec((1, width), whole),
                weight,
                weight,
                weight,
            ],
            out_specs=[
                pl.BlockSpec((1, rows, width), tile),
                pl.BlockSpec((width, 3 * inner), whole),
            ],
            scratch_shapes=[pltpu.VMEM((width, inner), jnp.float32)] * 3,
        ),
        out_shape=[
            jax.ShapeDtypeStruct((slots, rows, width), jnp.bfloat16),
            jax.ShapeDtypeStruct((width, 3 * inner), jnp.bfloat16),
        ],
        compiler_params=pltpu.CompilerParams(
            dimension_semantics=("arbitrary",), vmem_limit_bytes=48 * 1024 * 1024
        ),
    )(live, scale, x, cot, gain, w_value, w_gate, w_out)


def per_device(latents, cotangent, trunc_steps, timesteps, tile_map, gain, w_value, w_gate, w_out):
    slots, local_rows, width = latents.shape
    total = tile_map.shape[0]
    inner = w_value.shape[1]
    me = lax.axis_index("dp")
    live = jnp.clip(lax.dynamic_index_in_dim(trunc_steps, me, 0, keepdims=True) - 29, 1, slots)
    times = lax.dynamic_slice_in_dim(timesteps, me * slots, slots, 0)
    table = jnp.asarray(noise_table())
    scale = jnp.sum(
        jnp.where(times[:, None] == jnp.arange(1000, dtype=jnp.int32)[None, :], table[None, :], 0.0),
        axis=1,
    )
    full_x = lax.all_gather(latents, "tensor", axis=1, tiled=True)
    full_cot = lax.all_gather(cotangent, "tensor", axis=1, tiled=True)
    dn_part, dw_part = block_backward(
        live, scale, full_x, full_cot, gain[None, :], w_value, w_gate, w_out
    )
    d_normed = lax.psum_scatter(dn_part, "tensor", scatter_dimension=1, tiled=True)
    dw = lax.psum_scatter(dw_part, "dp", scatter_dimension=0, tiled=True).astype(jnp.float32)

    slot_live = (jnp.arange(slots, dtype=jnp.int32) < live[0])[:, None, None]
    d_normed = jnp.where(slot_live, d_normed.astype(jnp.float32), 0.0)
    x = latents.astype(jnp.float32)
    centred = x - jnp.mean(x, axis=-1, keepdims=True)
    inv_std = lax.rsqrt(jnp.mean(centred * centred, axis=-1, keepdims=True) + eps)
    x_hat = centred * inv_std
    grad = (cotangent.astype(jnp.float32) * scale[:, None, None]).astype(jnp.bfloat16)
    d_hat = d_normed * gain
    input_grad = grad.astype(jnp.float32) + inv_std * (
        d_hat
        - jnp.mean(d_hat, axis=-1, keepdims=True)
        - x_hat * jnp.mean(d_hat * x_hat, axis=-1, keepdims=True)
    )
    input_grad = jnp.where(slot_live, input_grad, 0.0).astype(jnp.bfloat16)
    grad_gain = lax.psum(jnp.sum(d_normed * x_hat, axis=(0, 1)), ("dp", "tensor"))

    item_ids = jnp.arange(total, dtype=jnp.int32)
    source = jnp.sum(
        jnp.where(tile_map[:, None] == item_ids[None, :], item_ids[:, None], 0), axis=0
    )
    pieces = lax.all_to_all(input_grad, "dp", split_axis=1, concat_axis=0, tiled=True)
    pieces = jnp.take(pieces, source, axis=0)
    placed = lax.all_to_all(pieces, "dp", split_axis=0, concat_axis=1, tiled=True)
    return (
        placed,
        dw[:, :inner],
        dw[:, inner : 2 * inner],
        dw[:, 2 * inner :],
        grad_gain,
    )


def solution(mesh):
    in_specs = (
        P("dp", "tensor", None),
        P("dp", "tensor", None),
        P(),
        P(),
        P(),
        P(),
        P(None, "tensor"),
        P(None, "tensor"),
        P(None, "tensor"),
    )
    out_specs = (
        P("dp", "tensor", None),
        P("dp", "tensor"),
        P("dp", "tensor"),
        P("dp", "tensor"),
        P(),
    )
    return jax.shard_map(
        per_device, mesh=mesh, in_specs=in_specs, out_specs=out_specs, check_vma=False
    )
```

```python
import functools

import jax
import jax.numpy as jnp
import numpy as np
from jax import lax
from jax.experimental import pallas as pl
from jax.experimental.pallas import tpu as pltpu
from jax.sharding import PartitionSpec as P

eps = 1e-05


def noise_table():
    betas = np.linspace(0.00085**0.5, 0.012**0.5, 1000) ** 2
    abar = np.exp(np.cumsum(np.log1p(-betas)))
    return np.sqrt(1.0 - abar).astype(np.float32)


def block_kernel(n, ahead, scale_ref, x_ref, cot_ref, gain_ref, wv_ref, wg_ref, wo_ref,
                 ig_ref, gg_ref, dw_ref,
                 full, part, other, acc_v, acc_g, acc_o, ag_send, ag_recv, rs_send, rs_recv):
    slots, rows, width = x_ref.shape
    inner = wv_ref.shape[1]
    me = lax.axis_index("tensor")
    high = n // 2
    my_high, my_low = me // 2, me % 2
    pair = my_high * 2 + (1 - my_low)
    line = [((my_high + k) % high) * 2 + my_low for k in range(1, high)]
    peers = [(me + k) % n for k in range(1, n)]
    first = (((0,), (0,)), ((), ()))
    last = (((1,), (1,)), ((), ()))
    local = (x_ref, cot_ref)

    def send(src, dst, send_sem, recv_sem, peer):
        return pltpu.make_async_remote_copy(
            src_ref=src, dst_ref=dst, send_sem=send_sem, recv_sem=recv_sem,
            device_id={"tensor": peer}, device_id_type=pl.DeviceIdType.MESH,
        )

    def own_copies(t):
        found = []
        for peer in [pair] + line:
            for kind in (0, 1):
                found.append(send(
                    local[kind].at[t], full.at[t, kind, me],
                    ag_send.at[t, len(found)], ag_recv.at[t, kind, me], peer,
                ))
        return found

    def passed_copies(t):
        found = []
        base = 2 * high
        for peer in line:
            found.append(send(
                full.at[t, 0, pair], full.at[t, 0, pair],
                ag_send.at[t, base + len(found)], ag_recv.at[t, 0, pair], peer,
            ))
        for owner in line:
            found.append(send(
                full.at[t, 1, owner], full.at[t, 1, owner],
                ag_send.at[t, base + len(found)], ag_recv.at[t, 1, owner], pair,
            ))
        return found

    def arrived(t, kind, owner):
        send(full.at[t, kind, owner], full.at[t, kind, owner], ag_send.at[t, 0],
             ag_recv.at[t, kind, owner], pair).wait_recv()

    def sum_copies(t):
        return [
            send(part.at[t, peer], other.at[t, me], rs_send.at[t, k], rs_recv.at[t, me], peer)
            for k, peer in enumerate(peers)
        ]

    def start_own(t):
        for copy in own_copies(t):
            copy.start()

    def pass_on(t):
        for owner in [pair] + line:
            for kind in (0, 1):
                arrived(t, kind, owner)
        for copy in passed_copies(t):
            copy.start()

    barrier = pltpu.get_barrier_semaphore()
    for peer in peers:
        pl.semaphore_signal(
            barrier, inc=1, device_id={"tensor": peer}, device_id_type=pl.DeviceIdType.MESH
        )
    pl.semaphore_wait(barrier, n - 1)
    for t in range(ahead):
        start_own(t)
    acc_v[...] = jnp.zeros_like(acc_v)
    acc_g[...] = jnp.zeros_like(acc_g)
    acc_o[...] = jnp.zeros_like(acc_o)
    gg_ref[...] = jnp.zeros_like(gg_ref)
    pass_on(0)

    def one_tile(t, carry):
        @pl.when(t + ahead < slots)
        def _():
            start_own(t + ahead)

        @pl.when(t + 1 < slots)
        def _():
            pass_on(t + 1)

        full[t, 0, me] = x_ref[t]
        full[t, 1, me] = cot_ref[t]
        far = [((my_high + k) % high) * 2 + (1 - my_low) for k in range(1, high)]
        for owner in far:
            for kind in (0, 1):
                arrived(t, kind, owner)
        x = full[t, 0].reshape(n * rows, width).astype(jnp.float32)
        centred = x - jnp.mean(x, axis=-1, keepdims=True)
        inv_std = lax.rsqrt(jnp.mean(centred * centred, axis=-1, keepdims=True) + eps)
        normed = (centred * inv_std * gain_ref[...]).astype(jnp.bfloat16)
        cot = full[t, 1].reshape(n * rows, width).astype(jnp.float32)
        grad = (cot * scale_ref[t]).astype(jnp.bfloat16)
        values = jnp.dot(normed, wv_ref[...], preferred_element_type=jnp.float32)
        gate = jnp.dot(normed, wg_ref[...], preferred_element_type=jnp.float32)
        d_hidden = jnp.dot(grad, wo_ref[...], preferred_element_type=jnp.float32)
        cdf = 0.5 * (1.0 + lax.erf(gate * 0.7071067811865476))
        density = jnp.exp(-0.5 * gate * gate) * 0.3989422804014327
        gelu = gate * cdf
        hidden = (values * gelu).astype(jnp.bfloat16)
        d_value = (d_hidden * gelu).astype(jnp.bfloat16)
        d_gate = (d_hidden * values * (cdf + gate * density)).astype(jnp.bfloat16)
        d_normed = lax.dot_general(d_value, wv_ref[...], last, preferred_element_type=jnp.float32)
        d_normed += lax.dot_general(d_gate, wg_ref[...], last, preferred_element_type=jnp.float32)
        part[t] = d_normed.astype(jnp.bfloat16).reshape(n, rows, width)
        for copy in sum_copies(t):
            copy.start()
        acc_v[...] += lax.dot_general(normed, d_value, first, preferred_element_type=jnp.float32)
        acc_g[...] += lax.dot_general(normed, d_gate, first, preferred_element_type=jnp.float32)
        acc_o[...] += lax.dot_general(grad, hidden, first, preferred_element_type=jnp.float32)
        return carry

    lax.fori_loop(0, slots, one_tile, 0)
    dw_ref[:, 0:inner] = acc_v[...].astype(jnp.bfloat16)
    dw_ref[:, inner : 2 * inner] = acc_g[...].astype(jnp.bfloat16)
    dw_ref[:, 2 * inner : 3 * inner] = acc_o[...].astype(jnp.bfloat16)

    def one_norm(t, carry):
        d_normed = part[t, me].astype(jnp.float32)
        for peer in peers:
            send(part.at[t, peer], other.at[t, peer], rs_send.at[t, 0], rs_recv.at[t, peer],
                 peer).wait_recv()
            d_normed += other[t, peer].astype(jnp.float32)
        x = x_ref[t].astype(jnp.float32)
        centred = x - jnp.mean(x, axis=-1, keepdims=True)
        inv_std = lax.rsqrt(jnp.mean(centred * centred, axis=-1, keepdims=True) + eps)
        x_hat = centred * inv_std
        grad = (cot_ref[t].astype(jnp.float32) * scale_ref[t]).astype(jnp.bfloat16)
        d_hat = d_normed * gain_ref[...]
        ig_ref[t] = (grad.astype(jnp.float32) + inv_std * (
            d_hat
            - jnp.mean(d_hat, axis=-1, keepdims=True)
            - x_hat * jnp.mean(d_hat * x_hat, axis=-1, keepdims=True)
        )).astype(jnp.bfloat16)
        gg_ref[...] += jnp.sum(d_normed * x_hat, axis=0, keepdims=True)
        for copy in own_copies(t) + passed_copies(t) + sum_copies(t):
            copy.wait_send()
        return carry

    lax.fori_loop(0, slots, one_norm, 0)


def block_backward(n, scale, x, cot, gain, w_value, w_gate, w_out):
    slots, rows, width = x.shape
    inner = w_value.shape[1]
    vmem = pl.BlockSpec(memory_space=pltpu.VMEM)
    sends = 2 * n // 2 + 2 * (n // 2 - 1)
    return pl.pallas_call(
        functools.partial(block_kernel, n, min(3, slots)),
        in_specs=[pl.BlockSpec(memory_space=pltpu.SMEM)] + [vmem] * 6,
        out_specs=[vmem] * 3,
        out_shape=[
            jax.ShapeDtypeStruct((slots, rows, width), jnp.bfloat16),
            jax.ShapeDtypeStruct((1, width), jnp.float32),
            jax.ShapeDtypeStruct((width, 3 * inner), jnp.bfloat16),
        ],
        scratch_shapes=[
            pltpu.VMEM((slots, 2, n, rows, width), jnp.bfloat16),
            pltpu.VMEM((slots, n, rows, width), jnp.bfloat16),
            pltpu.VMEM((slots, n, rows, width), jnp.bfloat16),
        ]
        + [pltpu.VMEM((width, inner), jnp.float32)] * 3
        + [
            pltpu.SemaphoreType.DMA((slots, sends)),
            pltpu.SemaphoreType.DMA((slots, 2, n)),
            pltpu.SemaphoreType.DMA((slots, n)),
            pltpu.SemaphoreType.DMA((slots, n)),
        ],
        compiler_params=pltpu.CompilerParams(
            collective_id=0, has_side_effects=True, vmem_limit_bytes=52 * 1024 * 1024
        ),
    )(scale, x, cot, gain, w_value, w_gate, w_out)


def per_device(latents, cotangent, trunc_steps, timesteps, tile_map, gain, w_value, w_gate, w_out):
    slots, local_rows, width = latents.shape
    total = tile_map.shape[0]
    inner = w_value.shape[1]
    me = lax.axis_index("dp")
    live = jnp.clip(lax.dynamic_index_in_dim(trunc_steps, me, 0, keepdims=True) - 29, 1, slots)
    times = lax.dynamic_slice_in_dim(timesteps, me * slots, slots, 0)
    table = jnp.asarray(noise_table())
    scale = jnp.sum(
        jnp.where(times[:, None] == jnp.arange(1000, dtype=jnp.int32)[None, :], table[None, :], 0.0),
        axis=1,
    )
    scale = jnp.where(jnp.arange(slots, dtype=jnp.int32) < live[0], scale, 0.0)
    input_grad, gain_part, dw_part = block_backward(
        lax.axis_size("tensor"), scale, latents, cotangent, gain[None, :], w_value, w_gate, w_out
    )
    grad_gain = lax.psum(gain_part[0], ("dp", "tensor"))
    dw = lax.psum_scatter(dw_part, "dp", scatter_dimension=0, tiled=True).astype(jnp.float32)

    item_ids = jnp.arange(total, dtype=jnp.int32)
    source = jnp.sum(
        jnp.where(tile_map[:, None] == item_ids[None, :], item_ids[:, None], 0), axis=0
    )
    pieces = lax.all_to_all(input_grad, "dp", split_axis=1, concat_axis=0, tiled=True)
    pieces = jnp.take(pieces, source, axis=0)
    placed = lax.all_to_all(pieces, "dp", split_axis=0, concat_axis=1, tiled=True)
    return (
        placed,
        dw[:, :inner],
        dw[:, inner : 2 * inner],
        dw[:, 2 * inner :],
        grad_gain,
    )


def solution(mesh):
    in_specs = (
        P("dp", "tensor", None),
        P("dp", "tensor", None),
        P(),
        P(),
        P(),
        P(),
        P(None, "tensor"),
        P(None, "tensor"),
        P(None, "tensor"),
    )
    out_specs = (
        P("dp", "tensor", None),
        P("dp", "tensor"),
        P("dp", "tensor"),
        P("dp", "tensor"),
        P(),
    )
    return jax.shard_map(
        per_device, mesh=mesh, in_specs=in_specs, out_specs=out_specs, check_vma=False
    )
```

```python
import functools

import jax
import jax.numpy as jnp
import numpy as np
from jax import lax
from jax.experimental import pallas as pl
from jax.experimental.pallas import tpu as pltpu
from jax.sharding import PartitionSpec as P

eps = 1e-05


def noise_table():
    betas = np.linspace(0.00085**0.5, 0.012**0.5, 1000) ** 2
    abar = np.exp(np.cumsum(np.log1p(-betas)))
    return np.sqrt(1.0 - abar).astype(np.float32)


def block_kernel(n, groups, ahead, lag, late, scale_ref, source_ref, x_ref, cot_ref, gain_ref,
                 wv_ref, wg_ref, wo_ref, ig_ref, gg_ref, dv_ref, dg_ref, do_ref,
                 full, part, other, acc_v, acc_g, acc_o, placed, gain_one, gain_two,
                 dw_part, dw_pair, dw_sum, dw_other,
                 ag_send, ag_recv, rs_send, rs_recv, out_send, out_recv,
                 gain_send, gain_recv, far_send, far_recv,
                 pair_send, pair_recv, sum_send, sum_recv):
    slots, rows, width = x_ref.shape
    inner = wv_ref.shape[1]
    me = lax.axis_index("tensor")
    high = n // 2
    my_high, my_low = me // 2, me % 2
    pair = my_high * 2 + (1 - my_low)
    line = [((my_high + k) % high) * 2 + my_low for k in range(1, high)]
    peers = [(me + k) % n for k in range(1, n)]
    first = (((0,), (0,)), ((), ()))
    last = (((1,), (1,)), ((), ()))
    local = (x_ref, cot_ref)
    group = lax.axis_index("dp")
    chips = groups // 2
    chip, core = group // 2, group % 2
    twin = chip * 2 + (1 - core)
    away = [((chip + k) % chips) for k in range(1, chips)]
    block = dw_part.shape[1]

    def cross(src, dst, send_sem, recv_sem, peer):
        return pltpu.make_async_remote_copy(
            src_ref=src, dst_ref=dst, send_sem=send_sem, recv_sem=recv_sem,
            device_id={"dp": peer}, device_id_type=pl.DeviceIdType.MESH,
        )

    def out_copy(t, owner, index, peer):
        spot = placed.at[owner * slots + t]
        return cross(spot, spot, out_send.at[t, index], out_recv.at[t, owner], peer)

    def out_own(t):
        found = [out_copy(t, group, k, c * 2 + core) for k, c in enumerate(away)]
        return found + [out_copy(t, group, chips - 1, twin)]

    def out_passed(t):
        return [out_copy(t, c * 2 + core, chips + k, twin) for k, c in enumerate(away)]

    def pass_out(t):
        for c, copy in zip(away, out_passed(t), strict=True):
            out_copy(t, c * 2 + core, 0, twin).wait_recv()
            copy.start()

    def send(src, dst, send_sem, recv_sem, peer):
        return pltpu.make_async_remote_copy(
            src_ref=src, dst_ref=dst, send_sem=send_sem, recv_sem=recv_sem,
            device_id={"tensor": peer}, device_id_type=pl.DeviceIdType.MESH,
        )

    def own_copies(t):
        found = []
        for peer in [pair] + line:
            for kind in (0, 1):
                found.append(send(
                    local[kind].at[t], full.at[t, kind, me],
                    ag_send.at[t, len(found)], ag_recv.at[t, kind, me], peer,
                ))
        return found

    def passed_copies(t):
        found = []
        base = 2 * high
        for peer in line:
            found.append(send(
                full.at[t, 0, pair], full.at[t, 0, pair],
                ag_send.at[t, base + len(found)], ag_recv.at[t, 0, pair], peer,
            ))
        for owner in line:
            found.append(send(
                full.at[t, 1, owner], full.at[t, 1, owner],
                ag_send.at[t, base + len(found)], ag_recv.at[t, 1, owner], pair,
            ))
        return found

    def arrived(t, kind, owner):
        send(full.at[t, kind, owner], full.at[t, kind, owner], ag_send.at[t, 0],
             ag_recv.at[t, kind, owner], pair).wait_recv()

    def sum_copies(t):
        return [
            send(part.at[t, peer], other.at[t, me], rs_send.at[t, k], rs_recv.at[t, me], peer)
            for k, peer in enumerate(peers)
        ]

    def start_own(t):
        for copy in own_copies(t):
            copy.start()

    def pass_on(t):
        for owner in [pair] + line:
            for kind in (0, 1):
                arrived(t, kind, owner)
        for copy in passed_copies(t):
            copy.start()

    barrier = pltpu.get_barrier_semaphore()
    for peer in peers:
        pl.semaphore_signal(
            barrier, inc=1, device_id={"tensor": peer}, device_id_type=pl.DeviceIdType.MESH
        )
    for k in range(1, groups):
        pl.semaphore_signal(
            barrier, inc=1, device_id={"dp": (group + k) % groups},
            device_id_type=pl.DeviceIdType.MESH,
        )
    pl.semaphore_wait(barrier, n - 1 + groups - 1)
    for t in range(ahead):
        start_own(t)
    acc_v[...] = jnp.zeros_like(acc_v)
    acc_g[...] = jnp.zeros_like(acc_g)
    acc_o[...] = jnp.zeros_like(acc_o)
    gg_ref[...] = jnp.zeros_like(gg_ref)
    pass_on(0)

    def finish(t):
        d_normed = part[t, me].astype(jnp.float32)
        for peer in peers:
            send(part.at[t, peer], other.at[t, peer], rs_send.at[t, 0], rs_recv.at[t, peer],
                 peer).wait_recv()
            d_normed += other[t, peer].astype(jnp.float32)
        x = x_ref[t].astype(jnp.float32)
        centred = x - jnp.mean(x, axis=-1, keepdims=True)
        inv_std = lax.rsqrt(jnp.mean(centred * centred, axis=-1, keepdims=True) + eps)
        x_hat = centred * inv_std
        grad = (cot_ref[t].astype(jnp.float32) * scale_ref[t]).astype(jnp.bfloat16)
        d_hat = d_normed * gain_ref[...]
        placed[group * slots + t] = (grad.astype(jnp.float32) + inv_std * (
            d_hat
            - jnp.mean(d_hat, axis=-1, keepdims=True)
            - x_hat * jnp.mean(d_hat * x_hat, axis=-1, keepdims=True)
        )).astype(jnp.bfloat16)
        for copy in out_own(t):
            copy.start()
        gg_ref[...] += jnp.sum(d_normed * x_hat, axis=0, keepdims=True)

    def one_tile(t, carry):
        @pl.when(t + ahead < slots)
        def _():
            start_own(t + ahead)

        @pl.when(t + 1 < slots)
        def _():
            pass_on(t + 1)

        full[t, 0, me] = x_ref[t]
        full[t, 1, me] = cot_ref[t]
        far = [((my_high + k) % high) * 2 + (1 - my_low) for k in range(1, high)]
        for owner in far:
            for kind in (0, 1):
                arrived(t, kind, owner)
        x = full[t, 0].reshape(n * rows, width).astype(jnp.float32)
        centred = x - jnp.mean(x, axis=-1, keepdims=True)
        inv_std = lax.rsqrt(jnp.mean(centred * centred, axis=-1, keepdims=True) + eps)
        normed = (centred * inv_std * gain_ref[...]).astype(jnp.bfloat16)
        cot = full[t, 1].reshape(n * rows, width).astype(jnp.float32)
        grad = (cot * scale_ref[t]).astype(jnp.bfloat16)
        values = jnp.dot(normed, wv_ref[...], preferred_element_type=jnp.float32)
        gate = jnp.dot(normed, wg_ref[...], preferred_element_type=jnp.float32)
        d_hidden = jnp.dot(grad, wo_ref[...], preferred_element_type=jnp.float32)
        cdf = 0.5 * (1.0 + lax.erf(gate * 0.7071067811865476))
        density = jnp.exp(-0.5 * gate * gate) * 0.3989422804014327
        gelu = gate * cdf
        hidden = (values * gelu).astype(jnp.bfloat16)
        d_value = (d_hidden * gelu).astype(jnp.bfloat16)
        d_gate = (d_hidden * values * (cdf + gate * density)).astype(jnp.bfloat16)
        d_normed = lax.dot_general(d_value, wv_ref[...], last, preferred_element_type=jnp.float32)
        d_normed += lax.dot_general(d_gate, wg_ref[...], last, preferred_element_type=jnp.float32)
        part[t] = d_normed.astype(jnp.bfloat16).reshape(n, rows, width)
        for copy in sum_copies(t):
            copy.start()
        acc_v[...] += lax.dot_general(normed, d_value, first, preferred_element_type=jnp.float32)
        acc_g[...] += lax.dot_general(normed, d_gate, first, preferred_element_type=jnp.float32)
        acc_o[...] += lax.dot_general(grad, hidden, first, preferred_element_type=jnp.float32)

        @pl.when(t >= lag)
        def _():
            finish(t - lag)

        @pl.when(t >= lag + late)
        def _():
            pass_out(t - lag - late)

        return carry

    lax.fori_loop(0, slots, one_tile, 0)
    for d in range(groups):
        rows_of = slice(d * block, (d + 1) * block)
        for k, acc in enumerate((acc_v, acc_g, acc_o)):
            dw_part[d, :, k * inner : (k + 1) * inner] = acc[rows_of, :].astype(jnp.bfloat16)
    pair_copies = [
        cross(dw_part.at[c * 2 + 1 - core], dw_pair.at[c], pair_send.at[c], pair_recv.at[c], twin)
        for c in range(chips)
    ]
    for copy in pair_copies:
        copy.start()

    def drain(t, carry):
        finish(t)
        return carry

    lax.fori_loop(slots - lag, slots, drain, 0)
    gain_one[me] = gg_ref[...]
    gain_copies = [
        send(gg_ref, gain_one.at[me], gain_send.at[k], gain_recv.at[me], peer)
        for k, peer in enumerate(peers)
    ]
    for copy in gain_copies:
        copy.start()
    for copy in pair_copies:
        copy.wait()
    for c in range(chips):
        both = dw_part[c * 2 + core].astype(jnp.float32) + dw_pair[c].astype(jnp.float32)
        dw_sum[c] = both.astype(jnp.bfloat16)
    sum_copies_z = [
        cross(dw_sum.at[c], dw_other.at[chip], sum_send.at[k], sum_recv.at[chip], c * 2 + core)
        for k, c in enumerate(away)
    ]
    for copy in sum_copies_z:
        copy.start()

    def drain_out(t, carry):
        pass_out(t)
        return carry

    lax.fori_loop(slots - lag - late, slots, drain_out, 0)
    for peer in peers:
        send(gg_ref, gain_one.at[peer], gain_send.at[0], gain_recv.at[peer], peer).wait_recv()
    for copy in gain_copies:
        copy.wait_send()
    gain_sum = gain_one[0]
    for k in range(1, n):
        gain_sum += gain_one[k]
    gain_two[group] = gain_sum
    far_copies = [
        cross(gain_two.at[group], gain_two.at[group], far_send.at[k], far_recv.at[group],
              (group + k) % groups)
        for k in range(1, groups)
    ]
    for copy in far_copies:
        copy.start()

    def settle(t, carry):
        for c in range(chips):
            out_copy(t, c * 2 + 1 - core, 0, twin).wait_recv()
        for copy in own_copies(t) + passed_copies(t) + sum_copies(t) + out_own(t) + out_passed(t):
            copy.wait_send()
        return carry

    lax.fori_loop(0, slots, settle, 0)

    def place(t, carry):
        ig_ref[t] = placed[source_ref[t]]
        return carry

    lax.fori_loop(0, slots, place, 0)
    for k in range(1, groups):
        peer = (group + k) % groups
        cross(gain_two.at[peer], gain_two.at[peer], far_send.at[k], far_recv.at[peer],
              peer).wait_recv()
    for copy in far_copies:
        copy.wait_send()
    gain_total = gain_two[0]
    for k in range(1, groups):
        gain_total += gain_two[k]
    gg_ref[...] = gain_total
    result = dw_sum[chip].astype(jnp.float32)
    for c in away:
        cross(dw_other.at[c], dw_other.at[c], sum_send.at[0], sum_recv.at[c], twin).wait_recv()
        result += dw_other[c].astype(jnp.float32)
    for copy in sum_copies_z:
        copy.wait_send()
    dv_ref[...] = result[:, 0:inner]
    dg_ref[...] = result[:, inner : 2 * inner]
    do_ref[...] = result[:, 2 * inner : 3 * inner]


def block_backward(n, groups, scale, source, x, cot, gain, w_value, w_gate, w_out):
    slots, rows, width = x.shape
    inner = w_value.shape[1]
    chips = groups // 2
    block = width // groups
    vmem = pl.BlockSpec(memory_space=pltpu.VMEM)
    smem = pl.BlockSpec(memory_space=pltpu.SMEM)
    grads = jax.ShapeDtypeStruct((block, inner), jnp.float32)
    dma = pltpu.SemaphoreType.DMA
    return pl.pallas_call(
        functools.partial(block_kernel, n, groups, 3, 2, 2),
        in_specs=[smem] * 2 + [vmem] * 6,
        out_specs=[vmem] * 5,
        out_shape=[
            jax.ShapeDtypeStruct((slots, rows, width), jnp.bfloat16),
            jax.ShapeDtypeStruct((1, width), jnp.float32),
            grads,
            grads,
            grads,
        ],
        scratch_shapes=[
            pltpu.VMEM((slots, 2, n, rows, width), jnp.bfloat16),
            pltpu.VMEM((slots, n, rows, width), jnp.bfloat16),
            pltpu.VMEM((slots, n, rows, width), jnp.bfloat16),
        ]
        + [pltpu.VMEM((width, inner), jnp.float32)] * 3
        + [
            pltpu.VMEM((groups * slots, rows, width), jnp.bfloat16),
            pltpu.VMEM((n, 1, width), jnp.float32),
            pltpu.VMEM((groups, 1, width), jnp.float32),
            pltpu.VMEM((groups, block, 3 * inner), jnp.bfloat16),
            pltpu.VMEM((chips, block, 3 * inner), jnp.bfloat16),
            pltpu.VMEM((chips, block, 3 * inner), jnp.bfloat16),
            pltpu.VMEM((chips, block, 3 * inner), jnp.bfloat16),
            dma((slots, n + 2 * (n // 2 - 1))),
            dma((slots, 2, n)),
            dma((slots, n)),
            dma((slots, n)),
            dma((slots, 2 * chips - 1)),
            dma((slots, groups)),
            dma((n,)),
            dma((n,)),
            dma((groups,)),
            dma((groups,)),
            dma((chips,)),
            dma((chips,)),
            dma((chips,)),
            dma((chips,)),
        ],
        compiler_params=pltpu.CompilerParams(
            collective_id=0, has_side_effects=True, vmem_limit_bytes=60 * 1024 * 1024
        ),
    )(scale, source, x, cot, gain, w_value, w_gate, w_out)


def per_device(latents, cotangent, trunc_steps, timesteps, tile_map, gain, w_value, w_gate, w_out):
    slots, local_rows, width = latents.shape
    total = tile_map.shape[0]
    inner = w_value.shape[1]
    me = lax.axis_index("dp")
    live = jnp.clip(lax.dynamic_index_in_dim(trunc_steps, me, 0, keepdims=True) - 29, 1, slots)
    times = lax.dynamic_slice_in_dim(timesteps, me * slots, slots, 0)
    table = jnp.asarray(noise_table())
    scale = jnp.sum(
        jnp.where(times[:, None] == jnp.arange(1000, dtype=jnp.int32)[None, :], table[None, :], 0.0),
        axis=1,
    )
    scale = jnp.where(jnp.arange(slots, dtype=jnp.int32) < live[0], scale, 0.0)
    item_ids = jnp.arange(total, dtype=jnp.int32)
    my_slots = me * slots + jnp.arange(slots, dtype=jnp.int32)
    source = jnp.sum(
        jnp.where(tile_map[:, None] == my_slots[None, :], item_ids[:, None], 0), axis=0
    )
    placed, grad_gain, grad_value, grad_gate, grad_out_proj = block_backward(
        lax.axis_size("tensor"), lax.axis_size("dp"), scale, source, latents, cotangent,
        gain[None, :], w_value, w_gate, w_out,
    )
    return (placed, grad_value, grad_gate, grad_out_proj, grad_gain[0])


def solution(mesh):
    in_specs = (
        P("dp", "tensor", None),
        P("dp", "tensor", None),
        P(),
        P(),
        P(),
        P(),
        P(None, "tensor"),
        P(None, "tensor"),
        P(None, "tensor"),
    )
    out_specs = (
        P("dp", "tensor", None),
        P("dp", "tensor"),
        P("dp", "tensor"),
        P("dp", "tensor"),
        P(),
    )
    return jax.shard_map(
        per_device, mesh=mesh, in_specs=in_specs, out_specs=out_specs, check_vma=False
    )
```
